32 devices in a mesh: rep: 1 (over z), mp: 4 (over y), tb: 4 (over x), ta: 2 (over core).
Axes of the slice: x: 4, y: 4, z: 1, core: 2. Of those that a mesh axis runs over, the one named last changes fastest.
The devices are a block of a 4x4x8 slice.
Arguments:
- tokens: bfloat16 [16384, 2048], P(('rep', 'ta', 'tb'), 'mp')
- seg_ids: int32 [16384], P(('rep', 'ta', 'tb'))
- positions: int32 [16384], P(('rep', 'ta', 'tb'))
- g_attn: bfloat16 [2, 2048], replicated
- w_q: bfloat16 [2, 2048, 2048], P(None, ('ta', 'tb'), 'mp')
- w_k: bfloat16 [2, 2048, 1024], P(None, ('ta', 'tb'), 'mp')
- w_v: bfloat16 [2, 2048, 1024], P(None, ('ta', 'tb'), 'mp')
- w_o: bfloat16 [2, 2048, 2048], P(None, 'mp', ('ta', 'tb'))
- g_mlp: bfloat16 [2, 2048], replicated
- w_gate: bfloat16 [2, 2048, 6144], P(None, ('ta', 'tb'), 'mp')
- w_up: bfloat16 [2, 2048, 6144], P(None, ('ta', 'tb'), 'mp')
- w_down: bfloat16 [2, 6144, 2048], P(None, 'mp', ('ta', 'tb'))
Outputs:
- output: float32 [16384, 2048], P(('rep', 'ta', 'tb'), 'mp')
All inputs are finite; a program needn't handle non-finite values.
Results may differ from the reference program's by a relative error of at most 0.0114562.
Values are sent between devices in bfloat16 or wider.
A program may use at most 768 MiB of HBM per device.

```python
import jax
import jax.numpy as jnp
from jax import lax

EMBED = 2048
HEADS = 16
KV_HEADS = 8
HEAD_DIM = 128
FFN_DIM = 6144
BLOCK_TOKENS = 2048
TOKEN_BLOCKS = 8
LAYERS = 2

TOTAL_TOKENS = TOKEN_BLOCKS * BLOCK_TOKENS
Q_PER_KV = HEADS // KV_HEADS


def draw_requests(req_key):
    cut_draw = jax.random.randint(req_key, (TOKEN_BLOCKS, BLOCK_TOKENS), 0, max(BLOCK_TOKENS // 4, 1))
    first_col = jnp.arange(BLOCK_TOKENS)[None, :] == 0
    starts = jnp.logical_or(cut_draw == 0, first_col)
    token_idx = jnp.arange(TOTAL_TOKENS, dtype=jnp.int32).reshape(TOKEN_BLOCKS, BLOCK_TOKENS)
    last_start = lax.cummax(jnp.where(starts, token_idx, 0), axis=1)
    positions = (token_idx - last_start).reshape(TOTAL_TOKENS)
    seg_ids = jnp.cumsum(starts.reshape(TOTAL_TOKENS).astype(jnp.int32)) - 1
    return seg_ids.astype(jnp.int32), positions.astype(jnp.int32)


def setup_inputs(seed: int = 0, part: int = 0) -> dict:
    base_key = jax.random.key(seed)
    part_key = jax.random.fold_in(base_key, part)
    tok_key, req_key = jax.random.split(part_key, 2)
    weight_keys = jax.random.split(base_key, 9)
    q_width = HEADS * HEAD_DIM
    kv_width = KV_HEADS * HEAD_DIM

    def normal_weight(draw_key, arr_shape, fan_in, scale_mult):
        values = jax.random.normal(draw_key, arr_shape, jnp.float32) * (scale_mult * fan_in ** -0.5)
        return values.astype(jnp.bfloat16)

    def gain_draw(draw_key):
        return jax.random.uniform(draw_key, (LAYERS, EMBED), jnp.float32, 0.5, 1.5).astype(jnp.bfloat16)

    tokens = jax.random.normal(tok_key, (TOTAL_TOKENS, EMBED), jnp.float32).astype(jnp.bfloat16)
    seg_ids, positions = draw_requests(req_key)
    return {
        'tokens': tokens,
        'seg_ids': seg_ids,
        'positions': positions,
        'g_attn': gain_draw(weight_keys[0]),
        'w_q': normal_weight(weight_keys[1], (LAYERS, EMBED, q_width), EMBED, 1.0),
        'w_k': normal_weight(weight_keys[2], (LAYERS, EMBED, kv_width), EMBED, 1.0),
        'w_v': normal_weight(weight_keys[3], (LAYERS, EMBED, kv_width), EMBED, 1.0),
        'w_o': normal_weight(weight_keys[4], (LAYERS, q_width, EMBED), q_width, 2.0),
        'g_mlp': gain_draw(weight_keys[5]),
        'w_gate': normal_weight(weight_keys[6], (LAYERS, EMBED, FFN_DIM), EMBED, 1.0),
        'w_up': normal_weight(weight_keys[7], (LAYERS, EMBED, FFN_DIM), EMBED, 1.0),
        'w_down': normal_weight(weight_keys[8], (LAYERS, FFN_DIM, EMBED), FFN_DIM, 1.0),
    }


def rms_norm(residual, gain_vec):
    mean_sq = jnp.mean(residual * residual, axis=-1, keepdims=True)
    return (residual * lax.rsqrt(mean_sq + 1e-6) * gain_vec.astype(jnp.float32)).astype(jnp.bfloat16)


def apply_rope(heads_in, positions):
    half_dim = HEAD_DIM // 2
    inv_freq = 10000.0 ** (-jnp.arange(half_dim, dtype=jnp.float32) * (2.0 / HEAD_DIM))
    angles = positions.astype(jnp.float32)[:, None] * inv_freq[None, :]
    cos_part = jnp.cos(angles)[:, None, :]
    sin_part = jnp.sin(angles)[:, None, :]
    low_half = heads_in[..., :half_dim].astype(jnp.float32)
    high_half = heads_in[..., half_dim:].astype(jnp.float32)
    rotated = jnp.concatenate([low_half * cos_part - high_half * sin_part, high_half * cos_part + low_half * sin_part], axis=-1)
    return rotated.astype(jnp.bfloat16)


def block_forward(block_in, weights):
    tokens_blk, seg_blk, pos_blk = block_in
    allowed = (seg_blk[:, None] == seg_blk[None, :]) & (pos_blk[None, :] <= pos_blk[:, None])
    score_scale = HEAD_DIM ** -0.5

    def kv_group_attention(group_in):
        q_grp, k_head, v_head = group_in
        scores = jnp.einsum('tgd,sd->gts', q_grp.astype(jnp.float32), k_head.astype(jnp.float32)) * score_scale
        attn_probs = jax.nn.softmax(jnp.where(allowed[None], scores, -1e30), axis=-1)
        return jnp.einsum('gts,sd->tgd', attn_probs, v_head.astype(jnp.float32)).astype(jnp.bfloat16)

    def layer_step(residual, layer_w):
        g_attn, w_q, w_k, w_v, w_o, g_mlp, w_gate, w_up, w_down = layer_w
        normed = rms_norm(residual, g_attn)
        queries = jnp.dot(normed, w_q, preferred_element_type=jnp.float32).astype(jnp.bfloat16)
        key_rows = jnp.dot(normed, w_k, preferred_element_type=jnp.float32).astype(jnp.bfloat16)
        value_rows = jnp.dot(normed, w_v, preferred_element_type=jnp.float32).astype(jnp.bfloat16)
        queries = apply_rope(queries.reshape(BLOCK_TOKENS, HEADS, HEAD_DIM), pos_blk)
        queries = queries.reshape(BLOCK_TOKENS, KV_HEADS, Q_PER_KV, HEAD_DIM)
        key_rows = apply_rope(key_rows.reshape(BLOCK_TOKENS, KV_HEADS, HEAD_DIM), pos_blk)
        value_rows = value_rows.reshape(BLOCK_TOKENS, KV_HEADS, HEAD_DIM)
        attn_out = lax.map(kv_group_attention, (jnp.transpose(queries, (1, 0, 2, 3)), jnp.transpose(key_rows, (1, 0, 2)), jnp.transpose(value_rows, (1, 0, 2))))
        attn_out = jnp.transpose(attn_out, (1, 0, 2, 3)).reshape(BLOCK_TOKENS, HEADS * HEAD_DIM)
        residual = residual + jnp.dot(attn_out, w_o, preferred_element_type=jnp.float32)
        normed = rms_norm(residual, g_mlp)
        gate_proj = jnp.dot(normed, w_gate, preferred_element_type=jnp.float32).astype(jnp.bfloat16)
        up_proj = jnp.dot(normed, w_up, preferred_element_type=jnp.float32).astype(jnp.bfloat16)
        mlp_act = (jax.nn.silu(gate_proj.astype(jnp.float32)) * up_proj.astype(jnp.float32)).astype(jnp.bfloat16)
        residual = residual + jnp.dot(mlp_act, w_down, preferred_element_type=jnp.float32)
        return residual, None

    final_state = lax.scan(layer_step, tokens_blk.astype(jnp.float32), weights)[0]
    return final_state


def reference(tokens, seg_ids, positions, g_attn, w_q, w_k, w_v, w_o, g_mlp, w_gate, w_up, w_down):
    weights = (g_attn, w_q, w_k, w_v, w_o, g_mlp, w_gate, w_up, w_down)
    blocks_in = (
        tokens.reshape(TOKEN_BLOCKS, BLOCK_TOKENS, EMBED),
        seg_ids.reshape(TOKEN_BLOCKS, BLOCK_TOKENS),
        positions.reshape(TOKEN_BLOCKS, BLOCK_TOKENS),
    )

    def run_block(block_in):
        return block_forward(block_in, weights)

    outputs = lax.map(run_block, blocks_in)
    return outputs.reshape(TOTAL_TOKENS, EMBED)
```

```python
import functools

import jax
import jax.numpy as jnp
from jax import lax
from jax.experimental import pallas as pl
from jax.experimental.pallas import tpu as pltpu
from jax.sharding import PartitionSpec as P

HEAD_DIM = 128
NORM_EPS = 1e-6
ROPE_BASE = 10000.0
SCORE_SCALE = HEAD_DIM ** -0.5
TOKEN_PLANE = ('ta', 'tb')
ATT_TILE = 512
BF16 = jnp.bfloat16
F32 = jnp.float32
VMEM_LIMIT = 56 * 1024 * 1024


def rope_tables(positions):
    half_dim = HEAD_DIM // 2
    inv_freq = ROPE_BASE ** (-jnp.arange(half_dim, dtype=F32) * (2.0 / HEAD_DIM))
    angles = positions.astype(F32)[:, None] * inv_freq
    cos_half, sin_half = jnp.cos(angles), jnp.sin(angles)
    return jnp.concatenate([cos_half, cos_half], -1), jnp.concatenate([-sin_half, sin_half], -1)


def rotate(rows, cos_rows, sin_rows):
    rows = rows.astype(F32)
    return (rows * cos_rows + pltpu.roll(rows, HEAD_DIM // 2, 1) * sin_rows).astype(BF16)


def attn_body(q_per_kv, lo_ref, q_ref, k_ref, v_ref, cos_ref, sin_ref, start_ref, out_ref, k_rot):
    tile = q_ref.shape[0]
    i = pl.program_id(1)

    @pl.when(i == 0)
    def _():
        def rot(c, carry):
            rows = pl.ds(pl.multiple_of(c * tile, tile), tile)
            k_rot[rows, :] = rotate(k_ref[rows, :], cos_ref[rows, :], sin_ref[rows, :])
            return carry
        lax.fori_loop(0, k_ref.shape[0] // tile, rot, 0)

    mine = pl.ds(pl.multiple_of(i * tile, tile), tile)
    cos_rows, sin_rows = cos_ref[mine, :], sin_ref[mine, :]
    row_id = i * tile + lax.broadcasted_iota(jnp.int32, (tile, tile), 0)
    col_id = lax.broadcasted_iota(jnp.int32, (tile, tile), 1)
    start = start_ref[mine, :]
    queries = [rotate(q_ref[:, g * HEAD_DIM:(g + 1) * HEAD_DIM], cos_rows, sin_rows) for g in range(q_per_kv)]

    def step(j, carry):
        rows = pl.ds(pl.multiple_of(j * tile, tile), tile)
        keys, values = k_rot[rows, :], v_ref[rows, :]
        cols = col_id + j * tile
        allowed = (cols <= row_id) & (cols >= start)
        new = []
        for g in range(q_per_kv):
            top, total, acc = carry[g]
            s = lax.dot_general(queries[g], keys, (((1,), (1,)), ((), ())), preferred_element_type=F32) * SCORE_SCALE
            s = jnp.where(allowed, s, -1e30)
            top_new = jnp.maximum(top, jnp.max(s, axis=-1, keepdims=True))
            p = jnp.exp(s - top_new)
            keep = jnp.exp(top - top_new)
            total = total * keep + jnp.sum(p, axis=-1, keepdims=True)
            acc = acc * keep + jnp.dot(p.astype(BF16), values, preferred_element_type=F32)
            new.append((top_new, total, acc))
        return tuple(new)

    init = tuple((jnp.full((tile, 1), -1e30, F32), jnp.zeros((tile, 1), F32), jnp.zeros((tile, HEAD_DIM), F32)) for _ in range(q_per_kv))
    done = lax.fori_loop(lo_ref[i], i + 1, step, init)
    for g in range(q_per_kv):
        _, total, acc = done[g]
        out_ref[:, g * HEAD_DIM:(g + 1) * HEAD_DIM] = (acc / total).astype(BF16)


def attention(qkv, n_q, n_kv, cos_tab, sin_tab, start, lo):
    rows = qkv.shape[0]
    q_per_kv = n_q // n_kv
    full = lambda off: pl.BlockSpec((rows, HEAD_DIM), lambda h, i, lo, off=off: (0, off + h))
    table = pl.BlockSpec((rows, HEAD_DIM), lambda h, i, lo: (0, 0))
    n_tiles = rows // ATT_TILE
    return pl.pallas_call(
        functools.partial(attn_body, q_per_kv),
        grid_spec=pltpu.PrefetchScalarGridSpec(
            num_scalar_prefetch=1,
            grid=(n_kv, n_tiles),
            in_specs=[
                pl.BlockSpec((ATT_TILE, q_per_kv * HEAD_DIM), lambda h, i, lo: (i, h)),
                full(n_q), full(n_q + n_kv), table, table,
                pl.BlockSpec((rows, 1), lambda h, i, lo: (0, 0)),
            ],
            out_specs=pl.BlockSpec((ATT_TILE, q_per_kv * HEAD_DIM), lambda h, i, lo: (i, h)),
            scratch_shapes=[pltpu.VMEM((rows, HEAD_DIM), BF16)],
        ),
        out_shape=jax.ShapeDtypeStruct((rows, n_q * HEAD_DIM), BF16),
        compiler_params=pltpu.CompilerParams(vmem_limit_bytes=VMEM_LIMIT, dimension_semantics=('arbitrary', 'arbitrary')),
        cost_estimate=pl.CostEstimate(flops=6 * rows * rows * HEAD_DIM * n_q, bytes_accessed=rows * HEAD_DIM * n_q * 6, transcendentals=rows * rows * n_q // 2),
        name='attn',
    )(lo, qkv, qkv, qkv, cos_tab, sin_tab, start)


def gate_up_body(h_ref, g_ref, u_ref, out_ref):
    h = h_ref[...]
    a = jnp.dot(h, g_ref[0], preferred_element_type=F32).astype(BF16).astype(F32)
    b = jnp.dot(h, u_ref[0], preferred_element_type=F32).astype(BF16).astype(F32)
    out_ref[...] = (a * jax.nn.sigmoid(a) * b).astype(BF16)


def gate_up(h, w):
    rows, depth = h.shape
    parts, _, both = w.shape
    cols = both // 2
    tile = 512
    n = cols // tile
    return pl.pallas_call(
        gate_up_body,
        grid=(parts, n),
        in_specs=[
            pl.BlockSpec((rows, depth), lambda p, j: (0, 0)),
            pl.BlockSpec((1, depth, tile), lambda p, j: (p, 0, j)),
            pl.BlockSpec((1, depth, tile), lambda p, j: (p, 0, n + j)),
        ],
        out_specs=pl.BlockSpec((rows, tile), lambda p, j: (0, p * n + j)),
        out_shape=jax.ShapeDtypeStruct((rows, parts * cols), BF16),
        compiler_params=pltpu.CompilerParams(vmem_limit_bytes=VMEM_LIMIT),
        cost_estimate=pl.CostEstimate(flops=2 * rows * depth * both * parts, bytes_accessed=2 * depth * both * parts, transcendentals=rows * cols * parts),
        name='gateup',
    )(h, w, w)


def out_body(x_ref, w_ref, out_ref):
    out_ref[...] = jnp.dot(x_ref[...], w_ref[0], preferred_element_type=F32)


def out_res_body(x_ref, w_ref, r_ref, out_ref):
    out_ref[...] = r_ref[...] + jnp.dot(x_ref[...], w_ref[0], preferred_element_type=F32)


def out_proj(x, w, resid=None):
    rows, depth = x.shape
    planes, _, cols = w.shape
    in_specs = [
        pl.BlockSpec((rows, depth), lambda p: (0, 0)),
        pl.BlockSpec((1, depth, cols), lambda p: (p, 0, 0)),
    ]
    args = [x, w]
    if resid is not None:
        in_specs.append(pl.BlockSpec((rows, cols), lambda p: (0, p)))
        args.append(resid)
    return pl.pallas_call(
        out_body if resid is None else out_res_body,
        grid=(planes,),
        in_specs=in_specs,
        out_specs=pl.BlockSpec((rows, cols), lambda p: (0, p)),
        out_shape=jax.ShapeDtypeStruct((rows, planes * cols), F32),
        compiler_params=pltpu.CompilerParams(vmem_limit_bytes=VMEM_LIMIT),
        cost_estimate=pl.CostEstimate(flops=2 * rows * depth * planes * cols, bytes_accessed=2 * depth * planes * cols, transcendentals=0),
        name='outproj',
    )(*args)


def down_body(n, plane_ref, x_ref, *refs):
    s, c = pl.program_id(0), pl.program_id(1)
    resid_ref, out_ref = refs[n], refs[n + 1]
    depth = refs[0].shape[0]
    rows = x_ref[:, pl.ds(pl.multiple_of(c * depth, depth), depth)]
    for k in range(n):
        @pl.when(s == k)
        def _(k=k):
            y = jnp.dot(rows, refs[k][...], preferred_element_type=F32)

            @pl.when(c == 0)
            def _():
                out_ref[...] = resid_ref[...] + y

            @pl.when(c > 0)
            def _():
                out_ref[...] += y


def down_proj(x, plane_of, pieces, resid):
    rows, depth = x.shape
    n = len(pieces)
    cols = pieces[0].shape[1]
    cuts = 2
    in_specs = [pl.BlockSpec((rows, depth), lambda s, c, planes: (0, 0))]
    for k in range(n):
        in_specs.append(pl.BlockSpec((depth // cuts, cols), lambda s, c, planes, k=k: (jnp.where(s == k, c, jnp.where(s < k, 0, cuts - 1)), 0)))
    tile = pl.BlockSpec((rows, cols), lambda s, c, planes: (0, planes[s]))
    return pl.pallas_call(
        functools.partial(down_body, n),
        grid_spec=pltpu.PrefetchScalarGridSpec(num_scalar_prefetch=1, grid=(n, cuts), in_specs=in_specs + [tile], out_specs=tile),
        out_shape=jax.ShapeDtypeStruct((rows, n * cols), F32),
        compiler_params=pltpu.CompilerParams(vmem_limit_bytes=VMEM_LIMIT),
        cost_estimate=pl.CostEstimate(flops=2 * rows * depth * n * cols, bytes_accessed=2 * depth * n * cols, transcendentals=0),
        name='downproj',
    )(plane_of, x, *pieces, resid)


def solution(mesh):
    mp_size = mesh.shape['mp']
    token_spec = P(('rep', 'ta', 'tb'), 'mp')
    id_spec = P(('rep', 'ta', 'tb'))
    in_proj_spec = P(None, TOKEN_PLANE, 'mp')
    out_proj_spec = P(None, 'mp', TOKEN_PLANE)
    gain_spec = P(None, None)
    up_ring = [(i, (i + 1) % mp_size) for i in range(mp_size)]
    down_ring = [(i, (i - 1) % mp_size) for i in range(mp_size)]
    fwd = lambda x: lax.ppermute(x, 'mp', up_ring)
    bwd = lambda x: lax.ppermute(x, 'mp', down_ring)
    x_size = mesh.shape['tb']
    x_fwd = lambda x: lax.ppermute(x, 'tb', [(i, (i + 1) % x_size) for i in range(x_size)])
    x_bwd = lambda x: lax.ppermute(x, 'tb', [(i, (i - 1) % x_size) for i in range(x_size)])

    def local_stack(tokens, seg_ids, positions, g_attn, w_q, w_k, w_v, w_o, g_mlp, w_gate, w_up, w_down):
        blk, embed_loc = tokens.shape
        embed = embed_loc * mp_size
        own = blk // mp_size
        me = lax.axis_index('mp')
        n_q = w_q.shape[2] // HEAD_DIM
        n_kv = w_k.shape[2] // HEAD_DIM
        layers = w_q.shape[0]

        def norm(rows, gain):
            mean_sq = jnp.sum(rows * rows, axis=-1, keepdims=True) / embed
            return (rows * lax.rsqrt(mean_sq + NORM_EPS) * gain.astype(F32)).astype(BF16)

        def gather(w, axes):
            return lax.all_gather(w, axes, axis=0, tiled=True)

        planes = mesh.shape['ta'] * mesh.shape['tb']
        w_qkv, w_out, w_gu = [], [], []
        for l in range(layers):
            w_qkv.append(gather(jnp.concatenate([w_q[l], w_k[l], w_v[l]], axis=1), TOKEN_PLANE))
            w_out.append(gather(w_o[l], TOKEN_PLANE + ('mp',)).reshape(planes, -1, w_o.shape[2]))
            gu = jnp.concatenate([w_gate[l], w_up[l]], axis=1)
            w_gu.append(gather(gu, ('mp',) + TOKEN_PLANE).reshape(mp_size, embed, -1))

        idx = jnp.arange(blk, dtype=jnp.int32)
        start = idx - positions
        lo = start[::ATT_TILE] // ATT_TILE
        start = start[:, None]
        cos_tab, sin_tab = rope_tables(positions)

        def ring_gather(x, fwd=fwd, bwd=bwd):
            prev, nxt = fwd(x), bwd(x)
            h = x.shape[0] // 2
            return prev, nxt, jnp.concatenate([fwd(prev[:h]), bwd(nxt[h:])], axis=0)

        def place(blocks, axis):
            size = blocks[0].shape[axis]
            shape = list(blocks[0].shape)
            shape[axis] = size * mp_size
            out = jnp.zeros(shape, blocks[0].dtype)
            for shift, b in zip((0, -1, 1, 2), blocks):
                where = lax.rem(me + shift + mp_size, mp_size) * size
                out = lax.dynamic_update_slice_in_dim(out, b, where, axis)
            return out

        tb, ta = lax.axis_index('tb'), lax.axis_index('ta')
        n_tb = mesh.shape['tb']
        other = lambda x: lax.ppermute(x, 'ta', [(0, 1), (1, 0)])
        dn_planes = jnp.stack([c * n_tb + lax.rem(tb + d, n_tb) for c in (ta, 1 - ta) for d in (0, n_tb - 1, 1, 2)]).astype(jnp.int32)

        def down_pieces(w):
            col = place((w,) + ring_gather(w), 0)
            mine = (col,) + ring_gather(col, x_fwd, x_bwd)
            return mine + tuple(other(p) for p in mine)

        w_dn = [down_pieces(w_down[0])]
        resid = None
        for l in range(layers):
            if l == 0:
                full = place((tokens,) + ring_gather(tokens), 1)
                resid = lax.dynamic_slice_in_dim(full, me * own, own, 0).astype(F32)
                h1 = norm(full.astype(F32), g_attn[l])
                qkv = jnp.dot(h1, w_qkv[l], preferred_element_type=F32).astype(BF16)
            else:
                h1 = norm(resid, g_attn[l])
                blocks = (h1,) + ring_gather(h1)
                qkv = place([jnp.dot(b, w_qkv[l], preferred_element_type=F32).astype(BF16) for b in blocks], 0)
            o = attention(qkv, n_q, n_kv, cos_tab, sin_tab, start, lo)
            o = lax.all_to_all(o, 'mp', split_axis=0, concat_axis=1, tiled=True)
            x1 = out_proj(o, w_out[l], resid)
            h2 = norm(x1, g_mlp[l])
            if l + 1 < layers:
                w_dn.append(down_pieces(lax.optimization_barrier((w_down[l + 1], x1))[0]))
            resid = down_proj(gate_up(h2, w_gu[l]), dn_planes, w_dn[l], x1)
        return lax.all_to_all(resid, 'mp', split_axis=1, concat_axis=0, tiled=True)

    return jax.shard_map(
        local_stack,
        mesh=mesh,
        in_specs=(token_spec, id_spec, id_spec, gain_spec, in_proj_spec, in_proj_spec, in_proj_spec, out_proj_spec, gain_spec, in_proj_spec, in_proj_spec, out_proj_spec),
        out_specs=token_spec,
        check_vma=False,
    )
```

```python
import functools
import math

import jax
import jax.numpy as jnp
from jax import lax
from jax.experimental import pallas as pl
from jax.experimental.pallas import tpu as pltpu
from jax.sharding import PartitionSpec as P

HEAD_DIM = 128
NORM_EPS = 1e-6
ROPE_BASE = 10000.0
EXP2_SCALE = HEAD_DIM ** -0.5 * math.log2(math.e)
TOKEN_PLANE = ('ta', 'tb')
ATT_TILE = 512
BF16 = jnp.bfloat16
F32 = jnp.float32
VMEM_LIMIT = 56 * 1024 * 1024


def rope_tables(positions):
    half_dim = HEAD_DIM // 2
    inv_freq = ROPE_BASE ** (-jnp.arange(half_dim, dtype=F32) * (2.0 / HEAD_DIM))
    angles = positions.astype(F32)[:, None] * inv_freq
    cos_half, sin_half = jnp.cos(angles), jnp.sin(angles)
    return jnp.concatenate([cos_half, cos_half], -1), jnp.concatenate([-sin_half, sin_half], -1)


def rotate(rows, cos_rows, sin_rows):
    rows = rows.astype(F32)
    return (rows * cos_rows + pltpu.roll(rows, HEAD_DIM // 2, 1) * sin_rows).astype(BF16)


def attn_body(q_per_kv, lo_ref, q_ref, k_ref, v_ref, cos_ref, sin_ref, start_ref, out_ref, k_rot):
    tile = q_ref.shape[0]
    i = pl.program_id(1)

    @pl.when(i == 0)
    def _():
        def rot(c, carry):
            rows = pl.ds(pl.multiple_of(c * tile, tile), tile)
            k_rot[rows, :] = rotate(k_ref[rows, :], cos_ref[rows, :], sin_ref[rows, :])
            return carry
        lax.fori_loop(0, k_ref.shape[0] // tile, rot, 0)

    mine = pl.ds(pl.multiple_of(i * tile, tile), tile)
    cos_rows, sin_rows = cos_ref[mine, :], sin_ref[mine, :]
    row_id = i * tile + lax.broadcasted_iota(jnp.int32, (tile, tile), 0)
    col_id = lax.broadcasted_iota(jnp.int32, (tile, tile), 1)
    start = start_ref[mine, :]
    queries = [rotate(q_ref[:, g * HEAD_DIM:(g + 1) * HEAD_DIM], cos_rows, sin_rows) for g in range(q_per_kv)]

    def step(j, carry):
        rows = pl.ds(pl.multiple_of(j * tile, tile), tile)
        keys = k_rot[rows, :]
        values = jnp.concatenate([v_ref[rows, :], jnp.ones((tile, HEAD_DIM), BF16)], axis=1)
        cols = col_id + j * tile
        allowed = (cols <= row_id) & (cols >= start)
        new = []
        for g in range(q_per_kv):
            top, acc = carry[g]
            s = lax.dot_general(queries[g], keys, (((1,), (1,)), ((), ())), preferred_element_type=F32)
            s = jnp.where(allowed, s, -1e30)
            top_new = jnp.maximum(top, jnp.max(s, axis=-1, keepdims=True))
            p = jnp.exp2((s - top_new) * EXP2_SCALE)
            keep = jnp.exp2((top - top_new) * EXP2_SCALE)
            acc = acc * keep + jnp.dot(p.astype(BF16), values, preferred_element_type=F32)
            new.append((top_new, acc))
        return tuple(new)

    init = tuple((jnp.full((tile, 1), -1e30, F32), jnp.zeros((tile, 2 * HEAD_DIM), F32)) for _ in range(q_per_kv))
    done = lax.fori_loop(lo_ref[i], i + 1, step, init)
    for g in range(q_per_kv):
        _, acc = done[g]
        out_ref[:, g * HEAD_DIM:(g + 1) * HEAD_DIM] = (acc[:, :HEAD_DIM] / acc[:, HEAD_DIM:]).astype(BF16)


def attention(qkv, n_q, n_kv, cos_tab, sin_tab, start, lo):
    rows = qkv.shape[0]
    q_per_kv = n_q // n_kv
    full = lambda off: pl.BlockSpec((rows, HEAD_DIM), lambda h, i, lo, off=off: (0, off + h))
    table = pl.BlockSpec((rows, HEAD_DIM), lambda h, i, lo: (0, 0))
    n_tiles = rows // ATT_TILE
    return pl.pallas_call(
        functools.partial(attn_body, q_per_kv),
        grid_spec=pltpu.PrefetchScalarGridSpec(
            num_scalar_prefetch=1,
            grid=(n_kv, n_tiles),
            in_specs=[
                pl.BlockSpec((ATT_TILE, q_per_kv * HEAD_DIM), lambda h, i, lo: (i, h)),
                full(n_q), full(n_q + n_kv), table, table,
                pl.BlockSpec((rows, 1), lambda h, i, lo: (0, 0)),
            ],
            out_specs=pl.BlockSpec((ATT_TILE, q_per_kv * HEAD_DIM), lambda h, i, lo: (i, h)),
            scratch_shapes=[pltpu.VMEM((rows, HEAD_DIM), BF16)],
        ),
        out_shape=jax.ShapeDtypeStruct((rows, n_q * HEAD_DIM), BF16),
        compiler_params=pltpu.CompilerParams(vmem_limit_bytes=VMEM_LIMIT, dimension_semantics=('arbitrary', 'arbitrary')),
        cost_estimate=pl.CostEstimate(flops=6 * rows * rows * HEAD_DIM * n_q, bytes_accessed=rows * HEAD_DIM * n_q * 6, transcendentals=rows * rows * n_q // 2),
        name='attn',
    )(lo, qkv, qkv, qkv, cos_tab, sin_tab, start)


def gate_up_body(h_ref, g_ref, u_ref, out_ref):
    h = h_ref[...]
    a = jnp.dot(h, g_ref[0], preferred_element_type=F32).astype(BF16).astype(F32)
    b = jnp.dot(h, u_ref[0], preferred_element_type=F32).astype(BF16).astype(F32)
    out_ref[...] = (a * jax.nn.sigmoid(a) * b).astype(BF16)


def gate_up(h, w):
    rows, depth = h.shape
    parts, _, both = w.shape
    cols = both // 2
    tile = 512
    n = cols // tile
    return pl.pallas_call(
        gate_up_body,
        grid=(parts, n),
        in_specs=[
            pl.BlockSpec((rows, depth), lambda p, j: (0, 0)),
            pl.BlockSpec((1, depth, tile), lambda p, j: (p, 0, j)),
            pl.BlockSpec((1, depth, tile), lambda p, j: (p, 0, n + j)),
        ],
        out_specs=pl.BlockSpec((rows, tile), lambda p, j: (0, p * n + j)),
        out_shape=jax.ShapeDtypeStruct((rows, parts * cols), BF16),
        compiler_params=pltpu.CompilerParams(vmem_limit_bytes=VMEM_LIMIT),
        cost_estimate=pl.CostEstimate(flops=2 * rows * depth * both * parts, bytes_accessed=2 * depth * both * parts, transcendentals=rows * cols * parts),
        name='gateup',
    )(h, w, w)


def out_body(x_ref, w_ref, out_ref):
    out_ref[...] = jnp.dot(x_ref[...], w_ref[0], preferred_element_type=F32)


def out_res_body(x_ref, w_ref, r_ref, out_ref):
    out_ref[...] = r_ref[...] + jnp.dot(x_ref[...], w_ref[0], preferred_element_type=F32)


def out_proj(x, w, resid=None):
    rows, depth = x.shape
    planes, _, cols = w.shape
    in_specs = [
        pl.BlockSpec((rows, depth), lambda p: (0, 0)),
        pl.BlockSpec((1, depth, cols), lambda p: (p, 0, 0)),
    ]
    args = [x, w]
    if resid is not None:
        in_specs.append(pl.BlockSpec((rows, cols), lambda p: (0, p)))
        args.append(resid)
    return pl.pallas_call(
        out_body if resid is None else out_res_body,
        grid=(planes,),
        in_specs=in_specs,
        out_specs=pl.BlockSpec((rows, cols), lambda p: (0, p)),
        out_shape=jax.ShapeDtypeStruct((rows, planes * cols), F32),
        compiler_params=pltpu.CompilerParams(vmem_limit_bytes=VMEM_LIMIT),
        cost_estimate=pl.CostEstimate(flops=2 * rows * depth * planes * cols, bytes_accessed=2 * depth * planes * cols, transcendentals=0),
        name='outproj',
    )(*args)


def down_body(n, plane_ref, x_ref, *refs):
    resid_ref, out_ref, slots, sems = refs[n:]
    s = pl.program_id(0)
    load = lambda k: pltpu.make_async_copy(refs[k], slots.at[k % 2], sems.at[k % 2])
    for k in range(n):
        @pl.when(s == k)
        def _(k=k):
            if k == 0:
                load(0).start()
            if k + 1 < n:
                load(k + 1).start()
            load(k).wait()
            out_ref[...] = resid_ref[...] + jnp.dot(x_ref[...], slots[k % 2], preferred_element_type=F32)


def down_proj(x, plane_of, pieces, resid):
    rows, depth = x.shape
    n = len(pieces)
    cols = pieces[0].shape[1]
    tile = pl.BlockSpec((rows, cols), lambda s, planes: (0, planes[s]))
    return pl.pallas_call(
        functools.partial(down_body, n),
        grid_spec=pltpu.PrefetchScalarGridSpec(
            num_scalar_prefetch=1,
            grid=(n,),
            in_specs=[pl.BlockSpec((rows, depth), lambda s, planes: (0, 0))] + [pl.BlockSpec(memory_space=pl.ANY)] * n + [tile],
            out_specs=tile,
            scratch_shapes=[pltpu.VMEM((2, depth, cols), BF16), pltpu.SemaphoreType.DMA((2,))],
        ),
        out_shape=jax.ShapeDtypeStruct((rows, n * cols), F32),
        compiler_params=pltpu.CompilerParams(vmem_limit_bytes=VMEM_LIMIT, dimension_semantics=('arbitrary',)),
        cost_estimate=pl.CostEstimate(flops=2 * rows * depth * n * cols, bytes_accessed=2 * depth * n * cols, transcendentals=0),
        name='downproj',
    )(plane_of, x, *pieces, resid)


def solution(mesh):
    mp_size = mesh.shape['mp']
    token_spec = P(('rep', 'ta', 'tb'), 'mp')
    id_spec = P(('rep', 'ta', 'tb'))
    in_proj_spec = P(None, TOKEN_PLANE, 'mp')
    out_proj_spec = P(None, 'mp', TOKEN_PLANE)
    gain_spec = P(None, None)
    up_ring = [(i, (i + 1) % mp_size) for i in range(mp_size)]
    down_ring = [(i, (i - 1) % mp_size) for i in range(mp_size)]
    fwd = lambda x: lax.ppermute(x, 'mp', up_ring)
    bwd = lambda x: lax.ppermute(x, 'mp', down_ring)
    x_size = mesh.shape['tb']
    x_fwd = lambda x: lax.ppermute(x, 'tb', [(i, (i + 1) % x_size) for i in range(x_size)])
    x_bwd = lambda x: lax.ppermute(x, 'tb', [(i, (i - 1) % x_size) for i in range(x_size)])

    def local_stack(tokens, seg_ids, positions, g_attn, w_q, w_k, w_v, w_o, g_mlp, w_gate, w_up, w_down):
        blk, embed_loc = tokens.shape
        embed = embed_loc * mp_size
        own = blk // mp_size
        me = lax.axis_index('mp')
        n_q = w_q.shape[2] // HEAD_DIM
        n_kv = w_k.shape[2] // HEAD_DIM
        layers = w_q.shape[0]

        def norm(rows, gain):
            mean_sq = jnp.sum(rows * rows, axis=-1, keepdims=True) / embed
            return (rows * lax.rsqrt(mean_sq + NORM_EPS) * gain.astype(F32)).astype(BF16)

        def gather(w, axes):
            return lax.all_gather(w, axes, axis=0, tiled=True)

        planes = mesh.shape['ta'] * mesh.shape['tb']
        w_qkv, w_out, w_gu = [], [], []
        for l in range(layers):
            w_qkv.append(gather(jnp.concatenate([w_q[l], w_k[l], w_v[l]], axis=1), TOKEN_PLANE))
            w_out.append(gather(w_o[l], TOKEN_PLANE + ('mp',)).reshape(planes, -1, w_o.shape[2]))
            gu = jnp.concatenate([w_gate[l], w_up[l]], axis=1)
            w_gu.append(gather(gu, ('mp',) + TOKEN_PLANE).reshape(mp_size, embed, -1))

        idx = jnp.arange(blk, dtype=jnp.int32)
        start = idx - positions
        lo = start[::ATT_TILE] // ATT_TILE
        start = start[:, None]
        cos_tab, sin_tab = rope_tables(positions)

        def ring_gather(x, fwd=fwd, bwd=bwd):
            prev, nxt = fwd(x), bwd(x)
            h = x.shape[0] // 2
            return prev, nxt, jnp.concatenate([fwd(prev[:h]), bwd(nxt[h:])], axis=0)

        def place(blocks, axis):
            size = blocks[0].shape[axis]
            shape = list(blocks[0].shape)
            shape[axis] = size * mp_size
            out = jnp.zeros(shape, blocks[0].dtype)
            for shift, b in zip((0, -1, 1, 2), blocks):
                where = lax.rem(me + shift + mp_size, mp_size) * size
                out = lax.dynamic_update_slice_in_dim(out, b, where, axis)
            return out

        tb, ta = lax.axis_index('tb'), lax.axis_index('ta')
        n_tb = mesh.shape['tb']
        other = lambda x: lax.ppermute(x, 'ta', [(0, 1), (1, 0)])
        dn_planes = jnp.stack([c * n_tb + lax.rem(tb + d, n_tb) for c in (ta, 1 - ta) for d in (0, n_tb - 1, 1, 2)]).astype(jnp.int32)

        def down_pieces(w):
            col = place((w,) + ring_gather(w), 0)
            mine = (col,) + ring_gather(col, x_fwd, x_bwd)
            return mine + tuple(other(p) for p in mine)

        w_dn = [down_pieces(w_down[0])]
        resid = None
        for l in range(layers):
            if l == 0:
                full = place((tokens,) + ring_gather(tokens), 1)
                resid = lax.dynamic_slice_in_dim(full, me * own, own, 0).astype(F32)
                h1 = norm(full.astype(F32), g_attn[l])
                qkv = jnp.dot(h1, w_qkv[l], preferred_element_type=F32).astype(BF16)
            else:
                h1 = norm(resid, g_attn[l])
                blocks = (h1,) + ring_gather(h1)
                qkv = place([jnp.dot(b, w_qkv[l], preferred_element_type=F32).astype(BF16) for b in blocks], 0)
            o = attention(qkv, n_q, n_kv, cos_tab, sin_tab, start, lo)
            o = lax.all_to_all(o, 'mp', split_axis=0, concat_axis=1, tiled=True)
            x1 = out_proj(o, w_out[l], resid)
            h2 = norm(x1, g_mlp[l])
            if l + 1 < layers:
                w_dn.append(down_pieces(lax.optimization_barrier((w_down[l + 1], x1))[0]))
            resid = down_proj(gate_up(h2, w_gu[l]), dn_planes, w_dn[l], x1)
        return lax.all_to_all(resid, 'mp', split_axis=1, concat_axis=0, tiled=True)

    return jax.shard_map(
        local_stack,
        mesh=mesh,
        in_specs=(token_spec, id_spec, id_spec, gain_spec, in_proj_spec, in_proj_spec, in_proj_spec, out_proj_spec, gain_spec, in_proj_spec, in_proj_spec, out_proj_spec),
        out_specs=token_spec,
        check_vma=False,
    )
```
